8 devices in a mesh: data: 1 (over z), tp: 8 (over y, x, core).
Axes of the slice: x: 2, y: 2, z: 1, core: 2. Of those that a mesh axis runs over, the one named last changes fastest.
Arguments:
- x: bfloat16 [8192, 32768], P('data', 'tp')
- w: bfloat16 [32768, 8192], P('tp')
- lengths: int32 [4], P('data')
Outputs:
- output: bfloat16 [8192, 8192], P('data')
All inputs are finite; a program needn't handle non-finite values.
Results may differ from the reference program's by a relative error of at most 0.001.
Values are sent between devices in bfloat16 or wider.
A program may use at most 1.25 GiB of HBM per device.

```python
import jax
import jax.numpy as jnp

D = 8192
FF = 32768
TOKENS = 8192
SEQS = 4
SEQ_LEN = TOKENS // SEQS


def draw_lengths(key_len):
    key_draw, key_perm = jax.random.split(key_len)
    lengths = jax.random.randint(key_draw, (SEQS,), 1, SEQ_LEN + 1, dtype=jnp.int32)
    slot_order = jax.random.permutation(key_perm, SEQS)
    lengths = lengths.at[slot_order[0]].set(SEQ_LEN)
    lengths = lengths.at[slot_order[1]].set(1)
    return lengths


def setup_inputs(seed: int = 0, part: int = 0) -> dict:
    key = jax.random.key(seed)
    key_x, key_w, key_len = jax.random.split(key, 3)
    tok_acts = jax.random.normal(jax.random.fold_in(key_x, part), (TOKENS, FF), jnp.float32)
    weight = jax.random.normal(key_w, (FF, D), jnp.float32) * (FF ** -0.5)
    lengths = draw_lengths(jax.random.fold_in(key_len, part))
    return {"x": tok_acts.astype(jnp.bfloat16), "w": weight.astype(jnp.bfloat16), "lengths": lengths}


def reference(x, w, lengths):
    seq_len = x.shape[0] // lengths.shape[0]
    valid = (jnp.arange(seq_len, dtype=jnp.int32)[None, :] < lengths[:, None]).reshape(-1)
    full_sum = jnp.dot(x, w, preferred_element_type=jnp.float32)
    return jnp.where(valid[:, None], full_sum, 0.0).astype(jnp.bfloat16)
```

```python
import functools

import jax
import jax.numpy as jnp
from jax import lax
from jax.experimental import pallas as pl
from jax.experimental.pallas import tpu as pltpu
from jax.sharding import PartitionSpec as P

MESH = pl.DeviceIdType.MESH
VMEM_LIMIT = 66_000_000
ALIGN = 8
ROWS = 256
TILE = 256
AHEAD = 4
WCOLS = 512


def compact_kernel(n_slots, seq_len, off_ref, len_ref, x_ref, xc_ref, buf, in_sem, out_sem):
    tiles = seq_len // TILE

    def valid(s, i):
        return i * TILE < len_ref[s]

    def read(s, i):
        b = (s % 2) * tiles + i
        return pltpu.make_async_copy(x_ref.at[pl.ds(s * seq_len + i * TILE, TILE)], buf.at[b], in_sem.at[b])

    def write(s, i):
        b = (s % 2) * tiles + i
        row = pl.multiple_of(off_ref[s] + i * TILE, ALIGN)
        return pltpu.make_async_copy(buf.at[b], xc_ref.at[pl.ds(row, TILE)], out_sem.at[b])

    def each(s, fn):
        for i in range(tiles):
            pl.when(valid(s, i))(functools.partial(fn, s, i))

    def flush(s, i):
        read(s, i).wait()
        write(s, i).start()

    each(0, lambda s, i: read(s, i).start())
    for s in range(n_slots):
        if s > 0:
            each(s - 1, lambda s, i: write(s, i).wait())
        if s + 1 < n_slots:
            each(s + 1, lambda s, i: read(s, i).start())
        each(s, flush)
    each(n_slots - 1, lambda s, i: write(s, i).wait())


def expand_kernel(n_slots, seq_len, off_ref, len_ref, yc_ref, y_ref, buf, zeros, in_sem, out_sem):
    per_slot = seq_len // TILE
    n_tiles = n_slots * per_slot
    ahead, n_buf = AHEAD, 2 * AHEAD
    zeros[...] = jnp.zeros_like(zeros)

    def left(k):
        return len_ref[k // per_slot] - (k % per_slot) * TILE

    def read(k):
        row = pl.multiple_of(off_ref[k // per_slot] + (k % per_slot) * TILE, ALIGN)
        return pltpu.make_async_copy(yc_ref.at[pl.ds(row, TILE)], buf.at[k % n_buf], in_sem.at[k % n_buf])

    def write(k, src):
        return pltpu.make_async_copy(src, y_ref.at[pl.ds(k * TILE, TILE)], out_sem.at[k % n_buf])

    for k in range(ahead):
        pl.when(left(k) > 0)(lambda k=k: read(k).start())

    def step(k, carry):
        nxt = k + ahead

        @pl.when(k >= n_buf - ahead)
        def _():
            write(k - (n_buf - ahead), zeros).wait()

        @pl.when(jnp.logical_and(nxt < n_tiles, left(jnp.minimum(nxt, n_tiles - 1)) > 0))
        def _():
            read(nxt).start()

        rest = left(k)

        @pl.when(rest > 0)
        def _():
            read(k).wait()

            @pl.when(rest < TILE)
            def _():
                def mask(i, c):
                    rows = pl.ds(pl.multiple_of(i * 16, 16), 16)
                    row_id = i * 16 + lax.broadcasted_iota(jnp.int32, (16, buf.shape[2]), 0)
                    old = buf[k % n_buf, rows, :].astype(jnp.float32)
                    buf[k % n_buf, rows, :] = jnp.where(row_id < rest, old, 0.0).astype(buf.dtype)
                    return c

                lax.fori_loop(0, TILE // 16, mask, 0)

            write(k, buf.at[k % n_buf]).start()

        @pl.when(rest <= 0)
        def _():
            write(k, zeros).start()

        return carry

    lax.fori_loop(0, n_tiles, step, 0)
    for k in range(n_tiles - (n_buf - ahead), n_tiles):
        write(k, zeros).wait()


def matmul_reduce_kernel(n, x_ref, w_ref, y_ref, xbuf, wbuf, part, d2r, r1, r2, yb,
                         x_sem, w_sem, ds_sem, dr_sem, s1_sem, r1_sem, s2_sem, r2_sem,
                         sg1_sem, rg1_sem, sg2_sem, rg2_sem, ol_sem, os_sem, or_sem):
    half_cols = part.shape[2]
    quart = half_cols // 2
    half_rows, quart_rows = ROWS // 2, ROWS // 4
    wt = half_cols // WCOLS
    me = lax.axis_index("tp")
    core, cx, cy = me % 2, (me // 2) % 2, me // 4
    pc, px, py = me + 1 - 2 * core, me + 2 - 4 * cx, me + 4 - 8 * cy
    first = ((cx, px), (cy, py))
    second = ((cy, py), (cx, px))
    cols = (pl.ds(0, quart), pl.ds(quart, quart))

    barrier = pltpu.get_barrier_semaphore()
    for dev in (pc, px, py):
        pl.semaphore_signal(barrier, inc=1, device_id={"tp": dev}, device_id_type=MESH)
    pl.semaphore_wait(barrier, 3)

    def remote(src, dst, send, recv, dev):
        return pltpu.make_async_remote_copy(src_ref=src, dst_ref=dst, send_sem=send, recv_sem=recv,
                                            device_id={"tp": dev}, device_id_type=MESH)

    def aligned(row, m):
        return pl.multiple_of(row, m)

    def load_x(c):
        return pltpu.make_async_copy(x_ref.at[pl.ds(aligned(c * ROWS, ROWS), ROWS)], xbuf.at[c % 2], x_sem.at[c % 2])

    def load_w(j):
        half = (1 - core + j // wt) % 2
        col = aligned(half * half_cols + (j % wt) * WCOLS, WCOLS)
        return pltpu.make_async_copy(w_ref.at[:, pl.ds(col, WCOLS)], wbuf.at[j % 2], w_sem.at[j % 2])

    def pair(c):
        return remote(part.at[3], d2r.at[c % 2], ds_sem, dr_sem.at[c % 2], pc)

    def base(h):
        return first[h][0] * half_rows

    def own(h):
        return aligned(base(h) + second[h][0] * quart_rows, quart_rows)

    def rs1(c, h):
        row = aligned((1 - first[h][0]) * half_rows, half_rows)
        return remote(part.at[c % 3, pl.ds(row, half_rows), cols[h]], r1.at[c % 3, h],
                      s1_sem.at[c % 2, h], r1_sem.at[c % 3, h], first[h][1])

    def rs2(c, h):
        row = aligned(base(h) + (1 - second[h][0]) * quart_rows, quart_rows)
        return remote(part.at[c % 3, pl.ds(row, quart_rows), cols[h]], r2.at[c % 3, h],
                      s2_sem.at[c % 2, h], r2_sem.at[c % 3, h], second[h][1])

    def ag1(c, h):
        ref = yb.at[c % 4, pl.ds(own(h), quart_rows), cols[h]]
        return remote(ref, ref, sg1_sem.at[c % 2, h], rg1_sem.at[c % 4, h], second[h][1])

    def ag2(c, h):
        ref = yb.at[c % 4, pl.ds(aligned(base(h), half_rows), half_rows), cols[h]]
        return remote(ref, ref, sg2_sem.at[c % 2, h], rg2_sem.at[c % 4, h], first[h][1])

    def place(c):
        return y_ref.at[pl.ds(aligned(c * ROWS, ROWS), ROWS), pl.ds(aligned(core * half_cols, half_cols), half_cols)]

    def out_local(c):
        return pltpu.make_async_copy(yb.at[c % 4], place(c), ol_sem)

    def out_pair(c):
        return remote(yb.at[c % 4], place(c), os_sem, or_sem.at[c % 2], pc)

    load_x(0).start()
    load_w(0).start()

    def step(t, carry):
        def stage(lag):
            c = t - lag
            return c, jnp.logical_and(c >= 0, c < n)

        c0, on = stage(6)

        @pl.when(on)
        def _():
            out_local(c0).wait()
            out_pair(c0).wait()

        c1, on = stage(1)

        @pl.when(on)
        def _():
            pair(c1).wait()

            def add(i, carry):
                rows = pl.ds(pl.multiple_of(i * 8, 8), 8)
                part[c1 % 3, rows, :] += d2r[c1 % 2, rows, :]
                return carry

            lax.fori_loop(0, ROWS // 8, add, 0)
            for h in range(2):
                rs1(c1, h).start()

        c2, on = stage(2)

        @pl.when(on)
        def _():
            for h in range(2):
                rs1(c2, h).wait()

                def add(i, carry, h=h):
                    rows = pl.ds(pl.multiple_of(base(h) + i * 8, 8), 8)
                    part[c2 % 3, rows, cols[h]] += r1[c2 % 3, h, pl.ds(pl.multiple_of(i * 8, 8), 8), :]
                    return carry

                lax.fori_loop(0, half_rows // 8, add, 0)
            for h in range(2):
                rs2(c2, h).start()

        c3, on = stage(3)

        @pl.when(on)
        def _():
            for h in range(2):
                rs2(c3, h).wait()

                def add(i, carry, h=h):
                    rows = pl.ds(pl.multiple_of(own(h) + i * 16, 16), 16)
                    total = part[c3 % 3, rows, cols[h]] + r2[c3 % 3, h, pl.ds(pl.multiple_of(i * 16, 16), 16), :]
                    yb[c3 % 4, rows, cols[h]] = total.astype(yb.dtype)
                    return carry

                lax.fori_loop(0, quart_rows // 16, add, 0)
            for h in range(2):
                ag1(c3, h).start()

        c4, on = stage(4)

        @pl.when(on)
        def _():
            for h in range(2):
                ag1(c4, h).wait()
            for h in range(2):
                ag2(c4, h).start()

        c5, on = stage(5)

        @pl.when(on)
        def _():
            for h in range(2):
                ag2(c5, h).wait()
            out_local(c5).start()
            out_pair(c5).start()

        @pl.when(t < n)
        def _():
            @pl.when(t + 1 < n)
            def _():
                load_x(t + 1).start()

            load_x(t).wait()

            def tile(j, carry):
                @pl.when(jnp.logical_or(j + 1 < 2 * wt, t + 1 < n))
                def _():
                    load_w((j + 1) % (2 * wt)).start()

                load_w(j).wait()

                @pl.when(j == wt)
                def _():
                    pair(t).start()

                slot = jnp.where(j < wt, 3, t % 3)
                col = pl.multiple_of((j % wt) * WCOLS, WCOLS)
                part[slot, :, pl.ds(col, WCOLS)] = jnp.dot(
                    xbuf[t % 2], wbuf[j % 2], preferred_element_type=jnp.float32)
                return carry

            lax.fori_loop(0, 2 * wt, tile, 0)

        return carry

    lax.fori_loop(0, n + 6, step, 0)


def solution(mesh):
    def any_spec():
        return pl.BlockSpec(memory_space=pl.ANY)

    def smem_spec():
        return pl.BlockSpec(memory_space=pltpu.SMEM)

    def local_part(x_loc, w_loc, lengths):
        tokens, depth = x_loc.shape
        width = w_loc.shape[1]
        n_slots = lengths.shape[0]
        seq_len = tokens // n_slots
        half = width // 2
        per_slot = seq_len // TILE
        least = seq_len + ALIGN * (n_slots - 1)
        most = (n_slots - 1) * seq_len + ALIGN
        lo, hi = -(-least // ROWS), -(-most // ROWS)
        counts = list(range(lo, hi + 1))
        cap = counts[-1] * ROWS

        padded = (lengths + (ALIGN - 1)) // ALIGN * ALIGN
        ends = jnp.cumsum(padded)
        offs = ends - padded
        chunks = (ends[-1] + (ROWS - 1)) // ROWS
        which = jnp.clip(chunks - lo, 0, len(counts) - 1)

        x_cmp = pl.pallas_call(
            functools.partial(compact_kernel, n_slots, seq_len),
            out_shape=jax.ShapeDtypeStruct((cap, depth), x_loc.dtype),
            in_specs=[smem_spec(), smem_spec(), any_spec()],
            out_specs=any_spec(),
            scratch_shapes=[
                pltpu.VMEM((2 * per_slot, TILE, depth), x_loc.dtype),
                pltpu.SemaphoreType.DMA((2 * per_slot,)),
                pltpu.SemaphoreType.DMA((2 * per_slot,)),
            ],
            compiler_params=pltpu.CompilerParams(vmem_limit_bytes=VMEM_LIMIT),
            name="compact",
        )(offs, lengths, x_loc)

        def branch(i, n, x_cmp, w_loc, offs, lengths):
            dma = pltpu.SemaphoreType.DMA
            y_cmp = pl.pallas_call(
                functools.partial(matmul_reduce_kernel, n),
                out_shape=jax.ShapeDtypeStruct((cap, width), jnp.bfloat16),
                in_specs=[any_spec(), any_spec()],
                out_specs=any_spec(),
                scratch_shapes=[
                    pltpu.VMEM((2, ROWS, depth), x_loc.dtype),
                    pltpu.VMEM((2, depth, WCOLS), w_loc.dtype),
                    pltpu.VMEM((4, ROWS, half), jnp.float32),
                    pltpu.VMEM((2, ROWS, half), jnp.float32),
                    pltpu.VMEM((3, 2, ROWS // 2, half // 2), jnp.float32),
                    pltpu.VMEM((3, 2, ROWS // 4, half // 2), jnp.float32),
                    pltpu.VMEM((4, ROWS, half), jnp.bfloat16),
                    dma((2,)), dma((2,)), dma, dma((2,)),
                    dma((2, 2)), dma((3, 2)), dma((2, 2)), dma((3, 2)),
                    dma((2, 2)), dma((4, 2)), dma((2, 2)), dma((4, 2)),
                    dma, dma, dma((2,)),
                ],
                compiler_params=pltpu.CompilerParams(
                    vmem_limit_bytes=VMEM_LIMIT, collective_id=i, has_side_effects=True),
                name=f"matmul_reduce_{n}",
            )(x_cmp, w_loc)
            return pl.pallas_call(
                functools.partial(expand_kernel, n_slots, seq_len),
                out_shape=jax.ShapeDtypeStruct((tokens, width), jnp.bfloat16),
                in_specs=[smem_spec(), smem_spec(), any_spec()],
                out_specs=any_spec(),
                scratch_shapes=[
                    pltpu.VMEM((2 * AHEAD, TILE, width), jnp.bfloat16),
                    pltpu.VMEM((TILE, width), jnp.bfloat16),
                    pltpu.SemaphoreType.DMA((2 * AHEAD,)),
                    pltpu.SemaphoreType.DMA((2 * AHEAD,)),
                ],
                compiler_params=pltpu.CompilerParams(vmem_limit_bytes=VMEM_LIMIT),
                name="expand",
            )(offs, lengths, y_cmp)

        branches = [functools.partial(branch, i, n) for i, n in enumerate(counts)]
        return lax.switch(which, branches, x_cmp, w_loc, offs, lengths)

    return jax.shard_map(local_part, mesh=mesh, in_specs=(P("data", "tp"), P("tp", None), P("data")),
                         out_specs=P("data", None), check_vma=False)
```

```python
import functools

import jax
import jax.numpy as jnp
from jax import lax
from jax.experimental import pallas as pl
from jax.experimental.pallas import tpu as pltpu
from jax.sharding import PartitionSpec as P

MESH = pl.DeviceIdType.MESH
VMEM_LIMIT = 66_000_000
ALIGN = 8
CHUNKS = (192, 256)
TILE = 128
AHEAD = 8
WCOLS = 512


def compact_kernel(n_slots, seq_len, off_ref, len_ref, x_ref, xc_ref, buf, in_sem, out_sem):
    tiles = seq_len // TILE

    def valid(s, i):
        return i * TILE < len_ref[s]

    def read(s, i):
        b = (s % 2) * tiles + i
        return pltpu.make_async_copy(x_ref.at[pl.ds(s * seq_len + i * TILE, TILE)], buf.at[b], in_sem.at[b])

    def write(s, i):
        b = (s % 2) * tiles + i
        row = pl.multiple_of(off_ref[s] + i * TILE, ALIGN)
        return pltpu.make_async_copy(buf.at[b], xc_ref.at[pl.ds(row, TILE)], out_sem.at[b])

    def each(s, fn):
        def one(i, carry):
            pl.when(valid(s, i))(functools.partial(fn, s, i))
            return carry

        lax.fori_loop(0, tiles, one, 0)

    def flush(s, i):
        read(s, i).wait()
        write(s, i).start()

    each(0, lambda s, i: read(s, i).start())
    for s in range(n_slots):
        if s > 0:
            each(s - 1, lambda s, i: write(s, i).wait())
        if s + 1 < n_slots:
            each(s + 1, lambda s, i: read(s, i).start())
        each(s, flush)
    each(n_slots - 1, lambda s, i: write(s, i).wait())


def expand_kernel(n_slots, seq_len, off_ref, len_ref, yc_ref, y_ref, buf, zeros, in_sem, out_sem):
    per_slot = seq_len // TILE
    n_tiles = n_slots * per_slot
    ahead, n_buf = AHEAD, 2 * AHEAD

    def clear(i, carry):
        zeros[pl.ds(pl.multiple_of(i * 16, 16), 16), :] = jnp.zeros((16, zeros.shape[1]), zeros.dtype)
        return carry

    lax.fori_loop(0, TILE // 16, clear, 0)

    def left(k):
        return len_ref[k // per_slot] - (k % per_slot) * TILE

    def read(k):
        row = pl.multiple_of(off_ref[k // per_slot] + (k % per_slot) * TILE, ALIGN)
        return pltpu.make_async_copy(yc_ref.at[pl.ds(row, TILE)], buf.at[k % n_buf], in_sem.at[k % n_buf])

    def write(k, src):
        return pltpu.make_async_copy(src, y_ref.at[pl.ds(k * TILE, TILE)], out_sem.at[k % n_buf])

    for k in range(ahead):
        pl.when(left(k) > 0)(lambda k=k: read(k).start())

    def step(k, carry):
        nxt = k + ahead

        @pl.when(k >= n_buf - ahead)
        def _():
            write(k - (n_buf - ahead), zeros).wait()

        @pl.when(jnp.logical_and(nxt < n_tiles, left(jnp.minimum(nxt, n_tiles - 1)) > 0))
        def _():
            read(nxt).start()

        rest = left(k)

        @pl.when(rest > 0)
        def _():
            read(k).wait()

            @pl.when(rest < TILE)
            def _():
                def mask(i, c):
                    rows = pl.ds(pl.multiple_of(i * 16, 16), 16)
                    row_id = i * 16 + lax.broadcasted_iota(jnp.int32, (16, buf.shape[2]), 0)
                    old = buf[k % n_buf, rows, :].astype(jnp.float32)
                    buf[k % n_buf, rows, :] = jnp.where(row_id < rest, old, 0.0).astype(buf.dtype)
                    return c

                lax.fori_loop(0, TILE // 16, mask, 0)

            write(k, buf.at[k % n_buf]).start()

        @pl.when(rest <= 0)
        def _():
            write(k, zeros).start()

        return carry

    lax.fori_loop(0, n_tiles, step, 0)
    for k in range(n_tiles - (n_buf - ahead), n_tiles):
        write(k, zeros).wait()


def matmul_reduce_kernel(n, x_ref, w_ref, y_ref, xbuf, wbuf, part, d2r, r1, r2, yb,
                         x_sem, w_sem, ds_sem, dr_sem, s1_sem, r1_sem, s2_sem, r2_sem,
                         sg1_sem, rg1_sem, sg2_sem, rg2_sem, ol_sem, os_sem, or_sem):
    n_rows, half_cols = part.shape[1:]
    quart = half_cols // 2
    half_rows, quart_rows = n_rows // 2, n_rows // 4
    wt = half_cols // WCOLS
    me = lax.axis_index("tp")
    core, cx, cy = me % 2, (me // 2) % 2, me // 4
    pc, px, py = me + 1 - 2 * core, me + 2 - 4 * cx, me + 4 - 8 * cy

    def first(h):
        return cx + h * (cy - cx), px + h * (py - px)

    def second(h):
        return cy + h * (cx - cy), py + h * (px - py)

    def cols(h):
        return pl.ds(pl.multiple_of(h * quart, quart), quart)

    def halves(fn):
        def one(h, carry):
            fn(h)
            return carry

        lax.fori_loop(0, 2, one, 0)

    barrier = pltpu.get_barrier_semaphore()
    for dev in (pc, px, py):
        pl.semaphore_signal(barrier, inc=1, device_id={"tp": dev}, device_id_type=MESH)
    pl.semaphore_wait(barrier, 3)

    def remote(src, dst, send, recv, dev):
        return pltpu.make_async_remote_copy(src_ref=src, dst_ref=dst, send_sem=send, recv_sem=recv,
                                            device_id={"tp": dev}, device_id_type=MESH)

    def aligned(row, m):
        return pl.multiple_of(row, m)

    def load_x(c):
        return pltpu.make_async_copy(x_ref.at[pl.ds(aligned(c * n_rows, 64), n_rows)], xbuf.at[c % 2], x_sem.at[c % 2])

    def piece(q):
        return pl.ds(aligned((q % 2) * quart + (q // 2) * WCOLS, WCOLS), WCOLS)

    def load_w(j):
        q, side = j // 2, j % 2
        half = (1 - core + side) % 2
        col = aligned(half * half_cols + (q % 2) * quart + (q // 2) * WCOLS, WCOLS)
        return pltpu.make_async_copy(w_ref.at[:, pl.ds(col, WCOLS)], wbuf.at[side], w_sem.at[side])

    def pair(c, q):
        return remote(part.at[3, :, piece(q)], d2r.at[c % 2, :, piece(q)], ds_sem.at[q], dr_sem.at[c % 2, q], pc)

    def pair_add(c, q):
        pair(c, q).wait()

        def add(i, carry):
            rows = pl.ds(pl.multiple_of(i * 32, 32), 32)
            part[c % 3, rows, piece(q)] += d2r[c % 2, rows, piece(q)]
            return carry

        lax.fori_loop(0, n_rows // 32, add, 0)

    def rs1_piece(c, q):
        h = q % 2
        own_first, dev = first(h)
        row = aligned((1 - own_first) * half_rows, 16)
        col = pl.ds(aligned((q // 2) * WCOLS, WCOLS), WCOLS)
        return remote(part.at[c % 3, pl.ds(row, half_rows), piece(q)], r1.at[c % 3, h, :, col],
                      s1_sem.at[c % 2, h], r1_sem.at[c % 3, h], dev)

    def base(h):
        return first(h)[0] * half_rows

    def own(h):
        return aligned(base(h) + second(h)[0] * quart_rows, 16)

    def rs1(c, h):
        row = aligned((1 - first(h)[0]) * half_rows, 16)
        return remote(part.at[c % 3, pl.ds(row, half_rows), cols(h)], r1.at[c % 3, h],
                      s1_sem.at[c % 2, h], r1_sem.at[c % 3, h], first(h)[1])

    def rs2(c, h):
        row = aligned(base(h) + (1 - second(h)[0]) * quart_rows, 16)
        return remote(part.at[c % 3, pl.ds(row, quart_rows), cols(h)], r2.at[c % 3, h],
                      s2_sem.at[c % 2, h], r2_sem.at[c % 3, h], second(h)[1])

    def ag1(c, h):
        ref = yb.at[c % 4, pl.ds(own(h), quart_rows), cols(h)]
        return remote(ref, ref, sg1_sem.at[c % 2, h], rg1_sem.at[c % 4, h], second(h)[1])

    def ag2(c, h):
        ref = yb.at[c % 4, pl.ds(aligned(base(h), 16), half_rows), cols(h)]
        return remote(ref, ref, sg2_sem.at[c % 2, h], rg2_sem.at[c % 4, h], first(h)[1])

    def place(c):
        return y_ref.at[pl.ds(aligned(c * n_rows, 64), n_rows), pl.ds(aligned(core * half_cols, half_cols), half_cols)]

    def out_local(c):
        return pltpu.make_async_copy(yb.at[c % 4], place(c), ol_sem)

    def out_pair(c):
        return remote(yb.at[c % 4], place(c), os_sem, or_sem.at[c % 6], pc)

    load_x(0).start()
    load_w(0).start()

    def step(t, carry):
        def stage(lag):
            c = t - lag
            return c, jnp.logical_and(c >= 0, c < n)

        c0, on = stage(6)

        @pl.when(on)
        def _():
            out_local(c0).wait()
            out_pair(c0).wait()

        c2, on = stage(2)

        @pl.when(on)
        def _():
            def take(h):
                rs1(c2, h).wait()

                def add(i, carry):
                    rows = pl.ds(pl.multiple_of(base(h) + i * 8, 8), 8)
                    part[c2 % 3, rows, cols(h)] += r1[c2 % 3, h, pl.ds(pl.multiple_of(i * 8, 8), 8), :]
                    return carry

                lax.fori_loop(0, half_rows // 8, add, 0)

            halves(take)
            halves(lambda h: rs2(c2, h).start())

        c3, on = stage(3)

        @pl.when(on)
        def _():
            def take(h):
                rs2(c3, h).wait()

                def add(i, carry):
                    rows = pl.ds(pl.multiple_of(own(h) + i * 16, 16), 16)
                    total = part[c3 % 3, rows, cols(h)] + r2[c3 % 3, h, pl.ds(pl.multiple_of(i * 16, 16), 16), :]
                    yb[c3 % 4, rows, cols(h)] = total.astype(yb.dtype)
                    return carry

                lax.fori_loop(0, quart_rows // 16, add, 0)

            halves(take)
            halves(lambda h: ag1(c3, h).start())

        c4, on = stage(4)

        @pl.when(on)
        def _():
            halves(lambda h: ag1(c4, h).wait())
            halves(lambda h: ag2(c4, h).start())

        c5, on = stage(5)

        @pl.when(on)
        def _():
            halves(lambda h: ag2(c5, h).wait())
            out_local(c5).start()
            out_pair(c5).start()

        @pl.when(t < n)
        def _():
            @pl.when(t + 1 < n)
            def _():
                load_x(t + 1).start()

            load_x(t).wait()

            def tile(j, carry):
                @pl.when(jnp.logical_or(j + 1 < 2 * wt, t + 1 < n))
                def _():
                    load_w((j + 1) % (2 * wt)).start()

                load_w(j).wait()
                q, side = j // 2, j % 2

                @pl.when(side == 1)
                def _():
                    pair(t, q).start()

                    @pl.when(q > 0)
                    def _():
                        rs1_piece(t, q - 1).start()

                slot = 3 + side * (t % 3 - 3)
                part[slot, :, piece(q)] = jnp.dot(
                    xbuf[t % 2], wbuf[side], preferred_element_type=jnp.float32)

                @pl.when(jnp.logical_and(side == 0, q > 0))
                def _():
                    pair_add(t, q - 1)

                return carry

            lax.fori_loop(0, 2 * wt, tile, 0)
            pair_add(t, wt - 1)
            rs1_piece(t, wt - 1).start()

        return carry

    lax.fori_loop(0, n + 6, step, 0)


def solution(mesh):
    def any_spec():
        return pl.BlockSpec(memory_space=pl.ANY)

    def smem_spec():
        return pl.BlockSpec(memory_space=pltpu.SMEM)

    def local_part(x_loc, w_loc, lengths):
        tokens, depth = x_loc.shape
        width = w_loc.shape[1]
        n_slots = lengths.shape[0]
        seq_len = tokens // n_slots
        half = width // 2
        per_slot = seq_len // TILE
        least = seq_len + ALIGN * (n_slots - 1)
        most = (n_slots - 1) * seq_len + ALIGN
        plans = {n * r: r for r in CHUNKS for n in range(-(-least // r), -(-most // r) + 1)}
        plans = sorted((total, r) for total, r in plans.items()
                       if r == CHUNKS[-1] or 4 * abs(2 * total - least - most) <= 3 * (most - least))
        cap = tokens

        padded = (lengths + (ALIGN - 1)) // ALIGN * ALIGN
        ends = jnp.cumsum(padded)
        offs = ends - padded
        totals = jnp.array([total for total, _ in plans], jnp.int32)
        which = jnp.minimum(jnp.sum((ends[-1] > totals).astype(jnp.int32)), len(plans) - 1)

        x_cmp = pl.pallas_call(
            functools.partial(compact_kernel, n_slots, seq_len),
            out_shape=jax.ShapeDtypeStruct((cap, depth), x_loc.dtype),
            in_specs=[smem_spec(), smem_spec(), any_spec()],
            out_specs=any_spec(),
            scratch_shapes=[
                pltpu.VMEM((2 * per_slot, TILE, depth), x_loc.dtype),
                pltpu.SemaphoreType.DMA((2 * per_slot,)),
                pltpu.SemaphoreType.DMA((2 * per_slot,)),
            ],
            compiler_params=pltpu.CompilerParams(vmem_limit_bytes=VMEM_LIMIT),
            name="compact",
        )(offs, lengths, x_loc)

        def branch(i, n, rows, x_cmp, w_loc):
            dma = pltpu.SemaphoreType.DMA
            y_cmp = pl.pallas_call(
                functools.partial(matmul_reduce_kernel, n),
                out_shape=jax.ShapeDtypeStruct((cap, width), jnp.bfloat16),
                in_specs=[any_spec(), any_spec()],
                out_specs=any_spec(),
                scratch_shapes=[
                    pltpu.VMEM((2, rows, depth), x_loc.dtype),
                    pltpu.VMEM((2, depth, WCOLS), w_loc.dtype),
                    pltpu.VMEM((4, rows, half), jnp.float32),
                    pltpu.VMEM((2, rows, half), jnp.float32),
                    pltpu.VMEM((3, 2, rows // 2, half // 2), jnp.float32),
                    pltpu.VMEM((3, 2, rows // 4, half // 2), jnp.float32),
                    pltpu.VMEM((4, rows, half), jnp.bfloat16),
                    dma((2,)), dma((2,)), dma((half // WCOLS,)), dma((2, half // WCOLS)),
                    dma((2, 2)), dma((3, 2)), dma((2, 2)), dma((3, 2)),
                    dma((2, 2)), dma((4, 2)), dma((2, 2)), dma((4, 2)),
                    dma, dma, dma((6,)),
                ],
                compiler_params=pltpu.CompilerParams(
                    vmem_limit_bytes=VMEM_LIMIT, collective_id=i, has_side_effects=True),
                name=f"matmul_reduce_{n}x{rows}",
            )(x_cmp, w_loc)
            return y_cmp

        branches = [functools.partial(branch, i, total // rows, rows) for i, (total, rows) in enumerate(plans)]
        y_cmp = lax.switch(which, branches, x_cmp, w_loc)
        return pl.pallas_call(
            functools.partial(expand_kernel, n_slots, seq_len),
            out_shape=jax.ShapeDtypeStruct((tokens, width), jnp.bfloat16),
            in_specs=[smem_spec(), smem_spec(), any_spec()],
            out_specs=any_spec(),
            scratch_shapes=[
                pltpu.VMEM((2 * AHEAD, TILE, width), jnp.bfloat16),
                pltpu.VMEM((TILE, width), jnp.bfloat16),
                pltpu.SemaphoreType.DMA((2 * AHEAD,)),
                pltpu.SemaphoreType.DMA((2 * AHEAD,)),
            ],
            compiler_params=pltpu.CompilerParams(vmem_limit_bytes=VMEM_LIMIT),
            name="expand",
        )(offs, lengths, y_cmp)

    return jax.shard_map(local_part, mesh=mesh, in_specs=(P("data", "tp"), P("tp", None), P("data")),
                         out_specs=P("data", None), check_vma=False)
```

```python
import functools

import jax
import jax.numpy as jnp
from jax import lax
from jax.experimental import pallas as pl
from jax.experimental.pallas import tpu as pltpu
from jax.sharding import PartitionSpec as P

MESH = pl.DeviceIdType.MESH
VMEM_LIMIT = 66_000_000
ALIGN = 8
CHUNKS = (192, 256)
TILE = 128
AHEAD = 8
WCOLS = 512


def compact_kernel(n_slots, seq_len, off_ref, len_ref, x_ref, xc_ref, buf, in_sem, out_sem):
    tiles = seq_len // TILE

    def valid(s, i):
        return i * TILE < len_ref[s]

    def read(s, i):
        b = (s % 2) * tiles + i
        return pltpu.make_async_copy(x_ref.at[pl.ds(s * seq_len + i * TILE, TILE)], buf.at[b], in_sem.at[b])

    def write(s, i):
        b = (s % 2) * tiles + i
        row = pl.multiple_of(off_ref[s] + i * TILE, ALIGN)
        return pltpu.make_async_copy(buf.at[b], xc_ref.at[pl.ds(row, TILE)], out_sem.at[b])

    def each(s, fn):
        def one(i, carry):
            pl.when(valid(s, i))(functools.partial(fn, s, i))
            return carry

        lax.fori_loop(0, tiles, one, 0)

    def flush(s, i):
        read(s, i).wait()
        write(s, i).start()

    each(0, lambda s, i: read(s, i).start())
    for s in range(n_slots):
        if s > 0:
            each(s - 1, lambda s, i: write(s, i).wait())
        if s + 1 < n_slots:
            each(s + 1, lambda s, i: read(s, i).start())
        each(s, flush)
    each(n_slots - 1, lambda s, i: write(s, i).wait())


def expand_kernel(n_slots, seq_len, off_ref, len_ref, yc_ref, y_ref, buf, zeros, in_sem, out_sem):
    per_slot = seq_len // TILE
    n_tiles = n_slots * per_slot
    ahead, n_buf = AHEAD, 2 * AHEAD

    def clear(i, carry):
        zeros[pl.ds(pl.multiple_of(i * 16, 16), 16), :] = jnp.zeros((16, zeros.shape[1]), zeros.dtype)
        return carry

    lax.fori_loop(0, TILE // 16, clear, 0)

    def left(k):
        return len_ref[k // per_slot] - (k % per_slot) * TILE

    def read(k):
        row = pl.multiple_of(off_ref[k // per_slot] + (k % per_slot) * TILE, ALIGN)
        return pltpu.make_async_copy(yc_ref.at[pl.ds(row, TILE)], buf.at[k % n_buf], in_sem.at[k % n_buf])

    def write(k, src):
        return pltpu.make_async_copy(src, y_ref.at[pl.ds(k * TILE, TILE)], out_sem.at[k % n_buf])

    for k in range(ahead):
        pl.when(left(k) > 0)(lambda k=k: read(k).start())

    def step(k, carry):
        nxt = k + ahead

        @pl.when(k >= n_buf - ahead)
        def _():
            write(k - (n_buf - ahead), zeros).wait()

        @pl.when(jnp.logical_and(nxt < n_tiles, left(jnp.minimum(nxt, n_tiles - 1)) > 0))
        def _():
            read(nxt).start()

        rest = left(k)

        @pl.when(rest > 0)
        def _():
            read(k).wait()

            @pl.when(rest < TILE)
            def _():
                def mask(i, c):
                    rows = pl.ds(pl.multiple_of(i * 16, 16), 16)
                    row_id = i * 16 + lax.broadcasted_iota(jnp.int32, (16, buf.shape[2]), 0)
                    old = buf[k % n_buf, rows, :].astype(jnp.float32)
                    buf[k % n_buf, rows, :] = jnp.where(row_id < rest, old, 0.0).astype(buf.dtype)
                    return c

                lax.fori_loop(0, TILE // 16, mask, 0)

            write(k, buf.at[k % n_buf]).start()

        @pl.when(rest <= 0)
        def _():
            write(k, zeros).start()

        return carry

    lax.fori_loop(0, n_tiles, step, 0)
    for k in range(n_tiles - (n_buf - ahead), n_tiles):
        write(k, zeros).wait()


def matmul_reduce_kernel(n, x_ref, w_ref, y_ref, xbuf, wbuf, part, d2r, r1, r2, yb,
                         x_sem, w_sem, ds_sem, dr_sem, s1_sem, r1_sem, s2_sem, r2_sem,
                         sg1_sem, rg1_sem, sg2_sem, rg2_sem, ol_sem, os_sem, or_sem):
    n_rows, half_cols = part.shape[1:]
    quart = half_cols // 2
    half_rows, quart_rows = n_rows // 2, n_rows // 4
    wt = half_cols // WCOLS
    me = lax.axis_index("tp")
    core, cx, cy = me % 2, (me // 2) % 2, me // 4
    pc, px, py = me + 1 - 2 * core, me + 2 - 4 * cx, me + 4 - 8 * cy

    def first(h):
        return cx + h * (cy - cx), px + h * (py - px)

    def second(h):
        return cy + h * (cx - cy), py + h * (px - py)

    def cols(h):
        return pl.ds(pl.multiple_of(h * quart, quart), quart)

    def halves(fn):
        def one(h, carry):
            fn(h)
            return carry

        lax.fori_loop(0, 2, one, 0)

    def remote(src, dst, send, recv, dev):
        return pltpu.make_async_remote_copy(src_ref=src, dst_ref=dst, send_sem=send, recv_sem=recv,
                                            device_id={"tp": dev}, device_id_type=MESH)

    def aligned(row, m):
        return pl.multiple_of(row, m)

    def load_x(c):
        return pltpu.make_async_copy(x_ref.at[pl.ds(aligned(c * n_rows, 64), n_rows)], xbuf.at[c % 2], x_sem.at[c % 2])

    def piece(q):
        return pl.ds(aligned((q % 2) * quart + (q // 2) * WCOLS, WCOLS), WCOLS)

    def load_w(k):
        j = k % (2 * wt)
        q, side = j // 2, j % 2
        half = (1 - core + side) % 2
        col = aligned(half * half_cols + (q % 2) * quart + (q // 2) * WCOLS, WCOLS)
        return pltpu.make_async_copy(w_ref.at[:, pl.ds(col, WCOLS)], wbuf.at[k % 3], w_sem.at[k % 3])

    def pair(c, q):
        return remote(part.at[3, :, piece(q)], d2r.at[c % 2, :, piece(q)], ds_sem.at[q], dr_sem.at[c % 2, q], pc)

    def pair_add(c, q):
        pair(c, q).wait()

        def add(i, carry):
            rows = pl.ds(pl.multiple_of(i * 32, 32), 32)
            part[c % 3, rows, piece(q)] += d2r[c % 2, rows, piece(q)]
            return carry

        lax.fori_loop(0, n_rows // 32, add, 0)

    def rs1_piece(c, q):
        h = q % 2
        own_first, dev = first(h)
        row = aligned((1 - own_first) * half_rows, 16)
        col = pl.ds(aligned((q // 2) * WCOLS, WCOLS), WCOLS)
        return remote(part.at[c % 3, pl.ds(row, half_rows), piece(q)], r1.at[c % 3, h, :, col],
                      s1_sem.at[c % 2, h], r1_sem.at[c % 3, h], dev)

    def base(h):
        return first(h)[0] * half_rows

    def own(h):
        return aligned(base(h) + second(h)[0] * quart_rows, 16)

    def rs1(c, h):
        row = aligned((1 - first(h)[0]) * half_rows, 16)
        return remote(part.at[c % 3, pl.ds(row, half_rows), cols(h)], r1.at[c % 3, h],
                      s1_sem.at[c % 2, h], r1_sem.at[c % 3, h], first(h)[1])

    def rs2(c, h):
        row = aligned(base(h) + (1 - second(h)[0]) * quart_rows, 16)
        return remote(part.at[c % 3, pl.ds(row, quart_rows), cols(h)], r2.at[c % 3, h],
                      s2_sem.at[c % 2, h], r2_sem.at[c % 3, h], second(h)[1])

    def ag1(c, h):
        ref = yb.at[c % 4, pl.ds(own(h), quart_rows), cols(h)]
        return remote(ref, ref, sg1_sem.at[c % 2, h], rg1_sem.at[c % 4, h], second(h)[1])

    def ag2(c, h):
        ref = yb.at[c % 4, pl.ds(aligned(base(h), 16), half_rows), cols(h)]
        return remote(ref, ref, sg2_sem.at[c % 2, h], rg2_sem.at[c % 4, h], first(h)[1])

    def place(c):
        return y_ref.at[pl.ds(aligned(c * n_rows, 64), n_rows), pl.ds(aligned(core * half_cols, half_cols), half_cols)]

    def out_local(c):
        return pltpu.make_async_copy(yb.at[c % 4], place(c), ol_sem)

    def out_pair(c):
        return remote(yb.at[c % 4], place(c), os_sem, or_sem.at[c % 6], pc)

    load_x(0).start()
    load_w(0).start()
    load_w(1).start()
    barrier = pltpu.get_barrier_semaphore()
    for dev in (pc, px, py):
        pl.semaphore_signal(barrier, inc=1, device_id={"tp": dev}, device_id_type=MESH)
    pl.semaphore_wait(barrier, 3)

    def step(t, carry):
        def stage(lag):
            c = t - lag
            return c, jnp.logical_and(c >= 0, c < n)

        c0, on = stage(6)

        @pl.when(on)
        def _():
            out_local(c0).wait()
            out_pair(c0).wait()

        c2, on = stage(2)

        @pl.when(on)
        def _():
            def take(h):
                rs1(c2, h).wait()

                def add(i, carry):
                    rows = pl.ds(pl.multiple_of(base(h) + i * 8, 8), 8)
                    part[c2 % 3, rows, cols(h)] += r1[c2 % 3, h, pl.ds(pl.multiple_of(i * 8, 8), 8), :]
                    return carry

                lax.fori_loop(0, half_rows // 8, add, 0)

            halves(take)
            halves(lambda h: rs2(c2, h).start())

        c3, on = stage(3)

        @pl.when(on)
        def _():
            def take(h):
                rs2(c3, h).wait()

                def add(i, carry):
                    rows = pl.ds(pl.multiple_of(own(h) + i * 16, 16), 16)
                    total = part[c3 % 3, rows, cols(h)] + r2[c3 % 3, h, pl.ds(pl.multiple_of(i * 16, 16), 16), :]
                    yb[c3 % 4, rows, cols(h)] = total.astype(yb.dtype)
                    return carry

                lax.fori_loop(0, quart_rows // 16, add, 0)

            halves(take)
            halves(lambda h: ag1(c3, h).start())

        c4, on = stage(4)

        @pl.when(on)
        def _():
            halves(lambda h: ag1(c4, h).wait())
            halves(lambda h: ag2(c4, h).start())

        c5, on = stage(5)

        @pl.when(on)
        def _():
            halves(lambda h: ag2(c5, h).wait())
            out_local(c5).start()
            out_pair(c5).start()

        @pl.when(t < n)
        def _():
            @pl.when(t + 1 < n)
            def _():
                load_x(t + 1).start()

            load_x(t).wait()

            def tile(j, carry):
                k = t * (2 * wt) + j

                @pl.when(k + 2 < n * 2 * wt)
                def _():
                    load_w(k + 2).start()

                load_w(k).wait()
                q, side = j // 2, j % 2

                @pl.when(side == 1)
                def _():
                    pair(t, q).start()

                    @pl.when(q > 0)
                    def _():
                        rs1_piece(t, q - 1).start()

                slot = 3 + side * (t % 3 - 3)
                part[slot, :, piece(q)] = jnp.dot(
                    xbuf[t % 2], wbuf[k % 3], preferred_element_type=jnp.float32)

                @pl.when(jnp.logical_and(side == 0, q > 0))
                def _():
                    pair_add(t, q - 1)

                return carry

            lax.fori_loop(0, 2 * wt, tile, 0)
            pair_add(t, wt - 1)
            rs1_piece(t, wt - 1).start()

        return carry

    lax.fori_loop(0, n + 6, step, 0)


def solution(mesh):
    def any_spec():
        return pl.BlockSpec(memory_space=pl.ANY)

    def smem_spec():
        return pl.BlockSpec(memory_space=pltpu.SMEM)

    def local_part(x_loc, w_loc, lengths):
        tokens, depth = x_loc.shape
        width = w_loc.shape[1]
        n_slots = lengths.shape[0]
        seq_len = tokens // n_slots
        half = width // 2
        per_slot = seq_len // TILE
        least = seq_len + ALIGN * (n_slots - 1)
        most = (n_slots - 1) * seq_len + ALIGN
        plans = {n * r: r for r in CHUNKS for n in range(-(-least // r), -(-most // r) + 1)}
        plans = sorted((total, r) for total, r in plans.items()
                       if r == CHUNKS[-1] or 4 * abs(2 * total - least - most) <= 3 * (most - least))
        cap = tokens

        padded = (lengths + (ALIGN - 1)) // ALIGN * ALIGN
        ends = jnp.cumsum(padded)
        offs = ends - padded
        totals = jnp.array([total for total, _ in plans], jnp.int32)
        which = jnp.minimum(jnp.sum((ends[-1] > totals).astype(jnp.int32)), len(plans) - 1)

        x_cmp = pl.pallas_call(
            functools.partial(compact_kernel, n_slots, seq_len),
            out_shape=jax.ShapeDtypeStruct((cap, depth), x_loc.dtype),
            in_specs=[smem_spec(), smem_spec(), any_spec()],
            out_specs=any_spec(),
            scratch_shapes=[
                pltpu.VMEM((2 * per_slot, TILE, depth), x_loc.dtype),
                pltpu.SemaphoreType.DMA((2 * per_slot,)),
                pltpu.SemaphoreType.DMA((2 * per_slot,)),
            ],
            compiler_params=pltpu.CompilerParams(vmem_limit_bytes=VMEM_LIMIT),
            name="compact",
        )(offs, lengths, x_loc)

        def branch(i, n, rows, x_cmp, w_loc):
            dma = pltpu.SemaphoreType.DMA
            y_cmp = pl.pallas_call(
                functools.partial(matmul_reduce_kernel, n),
                out_shape=jax.ShapeDtypeStruct((cap, width), jnp.bfloat16),
                in_specs=[any_spec(), any_spec()],
                out_specs=any_spec(),
                scratch_shapes=[
                    pltpu.VMEM((2, rows, depth), x_loc.dtype),
                    pltpu.VMEM((3, depth, WCOLS), w_loc.dtype),
                    pltpu.VMEM((4, rows, half), jnp.float32),
                    pltpu.VMEM((2, rows, half), jnp.float32),
                    pltpu.VMEM((3, 2, rows // 2, half // 2), jnp.float32),
                    pltpu.VMEM((3, 2, rows // 4, half // 2), jnp.float32),
                    pltpu.VMEM((4, rows, half), jnp.bfloat16),
                    dma((2,)), dma((3,)), dma((half // WCOLS,)), dma((2, half // WCOLS)),
                    dma((2, 2)), dma((3, 2)), dma((2, 2)), dma((3, 2)),
                    dma((2, 2)), dma((4, 2)), dma((2, 2)), dma((4, 2)),
                    dma, dma, dma((6,)),
                ],
                compiler_params=pltpu.CompilerParams(
                    vmem_limit_bytes=VMEM_LIMIT, collective_id=i, has_side_effects=True),
                name=f"matmul_reduce_{n}x{rows}",
            )(x_cmp, w_loc)
            return y_cmp

        branches = [functools.partial(branch, i, total // rows, rows) for i, (total, rows) in enumerate(plans)]
        y_cmp = lax.switch(which, branches, x_cmp, w_loc)
        return pl.pallas_call(
            functools.partial(expand_kernel, n_slots, seq_len),
            out_shape=jax.ShapeDtypeStruct((tokens, width), jnp.bfloat16),
            in_specs=[smem_spec(), smem_spec(), any_spec()],
            out_specs=any_spec(),
            scratch_shapes=[
                pltpu.VMEM((2 * AHEAD, TILE, width), jnp.bfloat16),
                pltpu.VMEM((TILE, width), jnp.bfloat16),
                pltpu.SemaphoreType.DMA((2 * AHEAD,)),
                pltpu.SemaphoreType.DMA((2 * AHEAD,)),
            ],
            compiler_params=pltpu.CompilerParams(vmem_limit_bytes=VMEM_LIMIT),
            name="expand",
        )(offs, lengths, y_cmp)

    return jax.shard_map(local_part, mesh=mesh, in_specs=(P("data", "tp"), P("tp", None), P("data")),
                         out_specs=P("data", None), check_vma=False)
```
